32 devices in a mesh: section: 8 (over z, y), dp: 2 (over x), spatial: 2 (over core).
Axes of the slice: x: 2, y: 2, z: 4, core: 2. Of those that a mesh axis runs over, the one named last changes fastest.
Arguments:
- inbox: bfloat16 [8, 4, 2, 256, 4, 128], P('section', None, 'dp', None, 'spatial'), may hold values from -6 to 6
- fresh: bfloat16 [3, 4, 2, 256, 4, 128], P(None, None, 'dp', None, 'spatial'), may hold values from -6 to 6
- params: float32 [8, 2, 9, 256, 256], P('section', None, None, ('dp', 'spatial')), may hold values from -6 to 6
- moments: float32 [8, 2, 9, 256, 256], P('section', None, None, ('dp', 'spatial')), may hold values from -3 to 3
Outputs:
- outbox: bfloat16 [8, 4, 2, 256, 4, 128], P('section', None, 'dp', None, 'spatial')
- params_out: float32 [8, 2, 9, 256, 256], P('section', None, None, ('dp', 'spatial'))
- moments_out: float32 [8, 2, 9, 256, 256], P('section', None, None, ('dp', 'spatial'))
The draws below stay inside these ranges and needn't reach their ends.
All inputs are finite; a program needn't handle non-finite values.
Results may differ from the reference program's by a relative error of at most 0.024.
Values may be sent and summed in bfloat16 or wider, within the bound.
No kernel may reach another device: no remote copies, remote signals or barrier semaphores. Data moves between devices by JAX's collectives and lax.ppermute only.
A program may use at most 64 MiB of HBM per device.

```python
import math
import jax
import jax.numpy as jnp
from jax import lax

C = 256
TICKS = 4
IMG_DEV = 1
ROW_DEV = 2
WCOL = 128
BLOCKS = 8
IMAGES = 2
ROWS = 4
N_DP = 2
N_SPATIAL = 2


def levels(stream_key, shape, pieces, smallest, top_value):
    def one(position, blocks):
        steps = jax.random.uniform(jax.random.fold_in(jax.random.fold_in(stream_key, 6), position), (blocks,), jnp.float32, smallest / len(pieces), top_value / len(pieces))
        return jnp.repeat(jnp.exp(steps), shape[position] // blocks).reshape((-1,) + (1,) * (len(shape) - position - 1))

    factor_of = one(*pieces[0])
    for cut in pieces[1:]:
        factor_of = factor_of * one(*cut)
    return factor_of


def centred(rng, shape, scale, limit, pieces=(), kind=jnp.bfloat16):
    values = jax.random.normal(rng, shape, jnp.float32) * scale
    if len(pieces) > 0:
        values = levels(rng, shape, pieces, -0.22, 0.18) * values
    return jnp.clip(values, min=-limit, max=limit).astype(kind)


def setup_inputs(seed: int = 0) -> dict:
    key_list = jax.random.split(jax.random.key(seed), 5)
    return {
        "inbox": centred(key_list[0], (BLOCKS, 4, IMAGES, C, ROWS, WCOL), 1.0, 6.0, ((0, 8), (2, 2), (4, 2))),
        "fresh": centred(key_list[1], (TICKS - 1, 4, IMAGES, C, ROWS, WCOL), 1.0, 6.0, ((2, 2), (4, 2))),
        "params": centred(key_list[2], (BLOCKS, 2, 9, C, C), 1.0, 6.0, ((0, 8), (3, 4)), jnp.float32),
        "moments": centred(key_list[3], (BLOCKS, 2, 9, C, C), 0.5, 3.0, ((0, 8), (3, 4)), jnp.float32),
    }


learn_rate = 0.05
momentum_decay = 0.9

def rounded(value):
    return lax.optimization_barrier(value.astype(jnp.bfloat16))

def silu_slope(value):
    sigma = jax.nn.sigmoid(value)
    return sigma * (1.0 + value * (1.0 - sigma))

def flipped(kernel):
    return jnp.swapaxes(kernel[::-1], 1, 2)

def conv_full(field, kernel):
    rows, cols = (field.shape[2], field.shape[3])
    padded = jnp.pad(field.astype(jnp.float32), ((0, 0), (0, 0), (1, 1), (1, 1)))
    weights = kernel.astype(jnp.float32)
    total = jnp.zeros((field.shape[0], kernel.shape[1], rows, cols), jnp.float32)
    for tap_row in range(3):
        for tap_col in range(3):
            window = padded[:, :, tap_row:tap_row + rows, tap_col:tap_col + cols]
            total = total + jnp.einsum('oc,ncrw->norw', weights[3 * tap_row + tap_col], window, precision=lax.Precision.HIGHEST)
    return total

def kernel_grad_full(cotangent, field):
    rows, cols = (field.shape[2], field.shape[3])
    padded = jnp.pad(field.astype(jnp.float32), ((0, 0), (0, 0), (1, 1), (1, 1)))
    grads = cotangent.astype(jnp.float32).reshape(N_DP, IMG_DEV, C, N_SPATIAL, ROW_DEV, WCOL)
    taps = []
    for tap_row in range(3):
        for tap_col in range(3):
            window = padded[:, :, tap_row:tap_row + rows, tap_col:tap_col + cols]
            window = window.reshape(N_DP, IMG_DEV, C, N_SPATIAL, ROW_DEV, WCOL)
            parts = jnp.einsum('gioshw,gicshw->gsoc', grads, window, precision=lax.Precision.HIGHEST)
            parts = lax.optimization_barrier(parts.astype(jnp.bfloat16)).astype(jnp.float32)
            taps.append(lax.optimization_barrier(jnp.sum(parts, axis=(0, 1))))
    return jnp.stack(taps)

def block_step(carried):
    message, kernels = carried
    half_one, half_two, grad_one, grad_two = (message[0], message[1], message[2], message[3])
    kernel_f, kernel_g = (kernels[0], kernels[1])
    act_one = rounded(jax.nn.silu(half_one.astype(jnp.float32)))
    prev_two = rounded(half_two.astype(jnp.float32) - conv_full(act_one, kernel_g))
    back_one = rounded(grad_one.astype(jnp.float32) + silu_slope(half_one.astype(jnp.float32)) * conv_full(grad_two, flipped(kernel_g)))
    act_two = rounded(jax.nn.silu(prev_two.astype(jnp.float32)))
    prev_one = rounded(half_one.astype(jnp.float32) - conv_full(act_two, kernel_f))
    back_two = rounded(grad_two.astype(jnp.float32) + silu_slope(prev_two.astype(jnp.float32)) * conv_full(back_one, flipped(kernel_f)))
    grad_g = kernel_grad_full(grad_two, act_one)
    grad_f = kernel_grad_full(back_one, act_two)
    sent = jnp.stack([prev_one, prev_two, back_one, back_two])
    return (sent, jnp.stack([grad_f, grad_g]))

def reference(inbox, fresh, params, moments):
    scale = 1.0 / math.sqrt(9 * C)
    message = inbox
    sent = inbox
    for tick_number in range(TICKS):
        if tick_number > 0:
            message = jnp.concatenate([sent[1:], fresh[tick_number - 1][None]], axis=0)
        kernels = (params * scale).astype(jnp.bfloat16)
        sent, grads = lax.map(block_step, (message, kernels))
        moments = momentum_decay * moments + scale * grads
        params = params - learn_rate * moments
    return (sent, params, moments)
```

```python
import functools
import math

import jax
import jax.numpy as jnp
from jax import lax
from jax.experimental import pallas as pl
from jax.experimental.pallas import tpu as pltpu
from jax.sharding import PartitionSpec as P

learn_rate = 0.05
momentum_decay = 0.9

VMEM = pl.BlockSpec(memory_space=pltpu.VMEM)
SMEM = pl.BlockSpec(memory_space=pltpu.SMEM)
f32 = jnp.float32
bf16 = jnp.bfloat16


def ring(axis, shift):
    count = lax.axis_size(axis)
    return [((i + shift) % count, i) for i in range(count)]


def around(shard, axis):
    return [shard] + [
        lax.ppermute(shard, axis, ring(axis, k)) for k in range(1, lax.axis_size(axis))
    ]


def silu_slope(value):
    sigma = jax.nn.sigmoid(value)
    return sigma * (1.0 + value * (1.0 - sigma))


def silu16(value):
    value = value.astype(f32)
    return (value * jax.nn.sigmoid(value)).astype(bf16)


def lane_shift(value, by):
    width = value.shape[-1]
    moved = pltpu.roll(value, by % width, 1)
    lane = lax.broadcasted_iota(jnp.int32, value.shape, 1)
    edge = 0 if by > 0 else width - 1
    return jnp.where(lane == edge, jnp.zeros_like(moved), moved)


def conv_rows(load, count, kernel):
    stacked = jnp.concatenate(
        [jnp.concatenate([load(r + a) for r in range(count)], axis=1) for a in range(3)], axis=0
    )
    sums = [jnp.dot(kernel[b], stacked, preferred_element_type=f32) for b in range(3)]
    width = stacked.shape[1] // count
    rows = []
    for r in range(count):
        left, middle, right = (s[:, r * width : (r + 1) * width] for s in sums)
        rows.append(middle + lane_shift(left, 1) + lane_shift(right, -1))
    return rows


def stage_one(pieces, place, *refs):
    first, second = refs[:pieces], refs[pieces : 2 * pieces]
    kernel, flip, padded_a, padded_b, own, raw, other = refs[2 * pieces :]
    band = first[0].shape[1]
    rows = band * pieces
    zero = jnp.zeros(padded_a.shape[2:], bf16)
    for member in range(2):
        for edge in (0, rows + 1):
            padded_a[member, edge] = zero
            padded_b[member, edge] = zero
    me = place[0]
    for s in range(pieces):
        start = lax.rem(me + s, pieces) * band
        for r in range(band):
            half = first[s][0, r]
            raw[start + r] = half
            padded_a[0, start + r + 1] = silu16(half)
            padded_a[1, start + r + 1] = first[s][1, r]
            for member in range(2):
                other[member, start + r] = second[s][member, r]
    moved = conv_rows(lambda i: padded_a[0, i], rows, kernel)
    for r in range(rows):
        prev = (other[0, r].astype(f32) - moved[r]).astype(bf16)
        other[0, r] = prev
        padded_b[0, r + 1] = silu16(prev)
    moved = conv_rows(lambda i: padded_a[1, i], rows, flip)
    for r in range(rows):
        slope = silu_slope(raw[r].astype(f32))
        back = (other[1, r].astype(f32) + slope * moved[r]).astype(bf16)
        other[1, r] = back
        padded_b[1, r + 1] = back
    for member in range(2):
        for r in range(band):
            own[member, r] = other[member, me * band + r]


def stage_two(place, padded, first, second, kernel, flip, out):
    band = first.shape[1]
    base = place[0] * band
    moved = conv_rows(lambda i: padded[0, base + i], band, kernel)
    for r in range(band):
        out[0, r] = (first[0, r].astype(f32) - moved[r]).astype(bf16)
    moved = conv_rows(lambda i: padded[1, base + i], band, flip)
    for r in range(band):
        slope = silu_slope(second[0, r].astype(f32))
        out[1, r] = (first[1, r].astype(f32) + slope * moved[r]).astype(bf16)


def update(pieces, images, final, scale, place, padded, *refs):
    count = pieces * (images - 1)
    given, refs = refs[:count], refs[count:]
    if final:
        params, moments, params_out, moments_out, act, cot, moved = refs
    else:
        (weights, speed, params, moments, weights_out, flip_out, speed_out, params_out,
         moments_out, act, cot, moved, total) = refs
    me, mine = place[0], place[1]
    rows = padded.shape[1] - 2
    band = rows // pieces
    channels = padded.shape[2]
    part = params.shape[1]
    for r in range(rows):
        act[r] = padded[0, r + 1]
        cot[r] = padded[1, r + 1]
    for image in range(images - 1):
        for s in range(pieces):
            piece = given[image * pieces + s]
            start = (image + 1) * rows + lax.rem(me + s, pieces) * band
            for r in range(band):
                act[start + r] = silu16(piece[0, r])
                cot[start + r] = piece[1, r]
    slot = pl.ds(pl.multiple_of(mine * part, part), part)
    for b in range(3):
        source = cot
        if b != 1:
            source = moved
            for r in range(images * rows):
                moved[r] = lane_shift(cot[r].astype(f32), b - 1).astype(bf16)
        for a in range(3):
            valid = [
                (i * rows + r, i * rows + r + a - 1)
                for i in range(images)
                for r in range(rows)
                if 0 <= r + a - 1 < rows
            ]
            if final:
                left = jnp.concatenate([source[r, slot, :] for r, _ in valid], axis=1)
            else:
                left = jnp.concatenate([source[r] for r, _ in valid], axis=1)
            right = jnp.concatenate([act[r] for _, r in valid], axis=1)
            grad = lax.dot_general(
                left, right, (((1,), (1,)), ((), ())), preferred_element_type=f32
            )
            tap = 3 * a + b
            if final:
                mine_grad = grad
            else:
                total[...] = grad
                mine_grad = total[slot, :]
            step = momentum_decay * moments[tap] + scale * mine_grad
            moments_out[tap] = step
            params_out[tap] = params[tap] - learn_rate * step
            if not final:
                cols = slice(a * channels, (a + 1) * channels)
                step = momentum_decay * speed[b, :, cols].astype(f32) + scale * grad
                speed_out[b, :, cols] = step.astype(bf16)
                fresh = weights[b, :, cols].astype(f32) - (learn_rate * scale) * step
                weights_out[b, :, cols] = fresh.astype(bf16)
                back = slice((2 - a) * channels, (3 - a) * channels)
                flip_out[2 - b, :, back] = fresh.T.astype(bf16)


def assemble(sections, pieces, flipping, place, *refs):
    count = sections * pieces
    given = refs[:count]
    out = refs[count]
    part, channels = given[0].shape[1:]
    me, at = place[0], place[2]
    for d in range(sections):
        for s in range(pieces):
            owner = lax.rem(at + d, sections) * pieces + lax.rem(me + s, pieces)
            slot = pl.ds(pl.multiple_of(owner * part, part), part)
            for a in range(3):
                for b in range(3):
                    out[b, slot, a * channels : (a + 1) * channels] = given[d * pieces + s][3 * a + b]
    if flipping:
        flip = refs[count + 1]
        for a in range(3):
            for b in range(3):
                block = out[b, :, a * channels : (a + 1) * channels].astype(f32)
                flip[2 - b, :, (2 - a) * channels : (3 - a) * channels] = block.T.astype(bf16)


def call(body, outs, inputs, flops, scratch=()):
    size = sum(math.prod(x.shape) * x.dtype.itemsize for x in list(inputs) + list(outs))
    return pl.pallas_call(
        body,
        out_shape=outs,
        in_specs=[SMEM] + [VMEM] * (len(inputs) - 1),
        out_specs=[VMEM] * len(outs),
        scratch_shapes=list(scratch),
        compiler_params=pltpu.CompilerParams(vmem_limit_bytes=32 * 1024 * 1024),
        cost_estimate=pl.CostEstimate(flops=flops, bytes_accessed=size, transcendentals=0),
    )(*inputs)


def local(inbox, fresh, params, moments):
    channels, band, width = inbox.shape[3:]
    scale = 1.0 / math.sqrt(9 * channels)
    pieces = lax.axis_size("spatial")
    images = lax.axis_size("dp")
    rows = band * pieces
    ticks = fresh.shape[0] + 1
    sections = lax.axis_size("section")
    top_section = lax.axis_index("section") == sections - 1
    me, at = lax.axis_index("spatial"), lax.axis_index("dp")
    place = jnp.stack([me, at * pieces + me, at]).astype(jnp.int32)
    shape = functools.partial(jax.ShapeDtypeStruct)
    message = shape((2, band, channels, width), bf16)
    padded = shape((2, rows + 2, channels, width), bf16)
    block = shape((3, channels, 3 * channels), bf16)
    conv_flops = 2 * 2 * 9 * channels * channels * rows * width
    share = params.shape[3]

    def rowwise(stack, members):
        return jnp.stack([jnp.swapaxes(stack[m, 0], 0, 1) for m in members])

    def gathered(shard, flipping):
        parts = [q for p in around(shard, "dp") for q in around(p, "spatial")]
        body = functools.partial(assemble, images, pieces, flipping)
        return call(body, [block] * (2 if flipping else 1), [place] + parts, channels**3)

    def one(first, second, kernel, flip):
        inputs = [place] + around(first, "spatial") + second + [kernel, flip]
        scratch = [pltpu.VMEM((rows, channels, width), bf16), pltpu.VMEM((2, rows, channels, width), bf16)]
        return call(
            functools.partial(stage_one, pieces), [padded, padded, message], inputs, conv_flops, scratch
        )

    def two(padded_b, first, second, kernel, flip):
        inputs = [place, padded_b, first, second, kernel, flip]
        return call(stage_two, [message], inputs, conv_flops // pieces)[0]

    def abroad(shard):
        return [q for p in around(shard, "dp")[1:] for q in around(p, "spatial")]

    def learn(padded_own, others, state, final):
        weights, speed, own_params, own_moments = state
        own = shape(own_params.shape, f32)
        field = pltpu.VMEM((images * rows, channels, width), bf16)
        scratch = [field] * 3
        outs = [own, own]
        inputs = [place, padded_own] + others
        if final:
            inputs += [own_params, own_moments]
        else:
            inputs += [weights, speed, own_params, own_moments]
            outs = [block] * 3 + outs
            scratch += [pltpu.VMEM((channels, channels), f32)]
        body = functools.partial(update, pieces, images, final, scale)
        flops = 2 * 9 * channels * channels * rows * width * images
        return call(body, outs, inputs, flops, scratch)

    first = rowwise(inbox[0], (0, 3))
    second = rowwise(inbox[0], (1, 2))
    kernels = (params[0] * scale).astype(bf16)
    speeds = moments[0].astype(bf16)
    weights_g, flip_g = gathered(kernels[1], True)
    weights_f, flip_f = gathered(kernels[0], True)
    (speed_g,) = gathered(speeds[1], False)
    (speed_f,) = gathered(speeds[0], False)
    params_f, params_g = params[0, 0], params[0, 1]
    moments_f, moments_g = moments[0, 0], moments[0, 1]
    down = [(i, i - 1) for i in range(1, sections)]
    second_all = around(second, "spatial")
    for tick in range(ticks):
        final = tick == ticks - 1
        padded_a, padded_b, middle = one(first, second_all, weights_g, flip_g)
        if not final:
            second = jnp.where(
                top_section, rowwise(fresh[tick], (1, 2)), lax.ppermute(middle, "section", down)
            )
            second_all = around(second, "spatial")
        last = two(padded_b, first, middle, weights_f, flip_f)
        others_g = abroad(first)
        others_f = abroad(middle)
        if not final:
            first = jnp.where(
                top_section, rowwise(fresh[tick], (0, 3)), lax.ppermute(last, "section", down)
            )
        state_g = (weights_g, speed_g, params_g, moments_g)
        state_f = (weights_f, speed_f, params_f, moments_f)
        if final:
            params_g, moments_g = learn(padded_a, others_g, state_g, True)
            params_f, moments_f = learn(padded_b, others_f, state_f, True)
        else:
            weights_g, flip_g, speed_g, params_g, moments_g = learn(padded_a, others_g, state_g, False)
            weights_f, flip_f, speed_f, params_f, moments_f = learn(padded_b, others_f, state_f, False)
    sent = jnp.stack([last[0], middle[0], middle[1], last[1]])
    outbox = jnp.swapaxes(sent, 1, 2)[None, :, None]
    return (
        outbox,
        jnp.stack([params_f, params_g])[None],
        jnp.stack([moments_f, moments_g])[None],
    )


def solution(mesh):
    placed = (
        P("section", None, "dp", None, "spatial", None),
        P(None, None, "dp", None, "spatial", None),
        P("section", None, None, ("dp", "spatial"), None),
        P("section", None, None, ("dp", "spatial"), None),
    )
    return jax.shard_map(
        local,
        mesh=mesh,
        in_specs=placed,
        out_specs=(
            P("section", None, "dp", None, "spatial", None),
            P("section", None, None, ("dp", "spatial"), None),
            P("section", None, None, ("dp", "spatial"), None),
        ),
        check_vma=False,
    )
```

```python
import functools
import math

import jax
import jax.numpy as jnp
from jax import lax
from jax.experimental import pallas as pl
from jax.experimental.pallas import tpu as pltpu
from jax.experimental.layout import Layout, with_layout_constraint
from jax.sharding import PartitionSpec as P


learn_rate = 0.05
momentum_decay = 0.9

VMEM = pl.BlockSpec(memory_space=pltpu.VMEM)
SMEM = pl.BlockSpec(memory_space=pltpu.SMEM)
f32 = jnp.float32
bf16 = jnp.bfloat16


def ring(axis, shift):
    count = lax.axis_size(axis)
    return [((i + shift) % count, i) for i in range(count)]


def around(shard, axis):
    return [shard] + [
        lax.ppermute(shard, axis, ring(axis, k)) for k in range(1, lax.axis_size(axis))
    ]


def silu_slope(value):
    sigma = jax.nn.sigmoid(value)
    return sigma * (1.0 + value * (1.0 - sigma))


def silu16(value):
    value = value.astype(f32)
    return (value * jax.nn.sigmoid(value)).astype(bf16)


def lane_shift(value, by):
    width = value.shape[-1]
    moved = pltpu.roll(value, by % width, 1)
    lane = lax.broadcasted_iota(jnp.int32, value.shape, 1)
    edge = 0 if by > 0 else width - 1
    return jnp.where(lane == edge, jnp.zeros_like(moved), moved)


def conv_rows(load, count, kernel):
    stacked = jnp.concatenate(
        [jnp.concatenate([load(r + a) for r in range(count)], axis=1) for a in range(3)], axis=0
    )
    sums = [jnp.dot(kernel[b], stacked, preferred_element_type=f32) for b in range(3)]
    width = stacked.shape[1] // count
    rows = []
    for r in range(count):
        left, middle, right = (s[:, r * width : (r + 1) * width] for s in sums)
        rows.append(middle + lane_shift(left, 1) + lane_shift(right, -1))
    return rows


def stage_one(pieces, place, *refs):
    first, second = refs[:pieces], refs[pieces : 2 * pieces]
    kernel, flip, padded_a, padded_b, own, raw, other = refs[2 * pieces :]
    band = first[0].shape[1]
    rows = band * pieces
    zero = jnp.zeros(padded_a.shape[2:], bf16)
    for member in range(2):
        for edge in (0, rows + 1):
            padded_a[member, edge] = zero
            padded_b[member, edge] = zero
    me = place[0]
    for s in range(pieces):
        start = lax.rem(me + s, pieces) * band
        for r in range(band):
            half = first[s][0, r]
            raw[start + r] = half
            padded_a[0, start + r + 1] = silu16(half)
            padded_a[1, start + r + 1] = first[s][1, r]
            for member in range(2):
                other[member, start + r] = second[s][member, r]
    moved = conv_rows(lambda i: padded_a[0, i], rows, kernel)
    for r in range(rows):
        prev = (other[0, r].astype(f32) - moved[r]).astype(bf16)
        other[0, r] = prev
        padded_b[0, r + 1] = silu16(prev)
    moved = conv_rows(lambda i: padded_a[1, i], rows, flip)
    for r in range(rows):
        slope = silu_slope(raw[r].astype(f32))
        back = (other[1, r].astype(f32) + slope * moved[r]).astype(bf16)
        other[1, r] = back
        padded_b[1, r + 1] = back
    for member in range(2):
        for r in range(band):
            own[member, r] = other[member, me * band + r]


def stage_two(place, padded, first, second, kernel, flip, out):
    band = first.shape[1]
    base = place[0] * band
    moved = conv_rows(lambda i: padded[0, base + i], band, kernel)
    for r in range(band):
        out[0, r] = (first[0, r].astype(f32) - moved[r]).astype(bf16)
    moved = conv_rows(lambda i: padded[1, base + i], band, flip)
    for r in range(band):
        slope = silu_slope(second[0, r].astype(f32))
        out[1, r] = (first[1, r].astype(f32) + slope * moved[r]).astype(bf16)


def update(pieces, images, final, scale, place, padded, *refs):
    count = pieces * (images - 1)
    given, refs = refs[:count], refs[count:]
    if final:
        params, moments = refs[:2]
        params_out, moments_out, act, cot, moved = refs[-5:]
        params_out, moments_out = params_out.at[0], moments_out.at[0]
    else:
        (weights, speed, params, moments, weights_out, flip_out, speed_out, params_out,
         moments_out, act, cot, moved, total) = refs
    me, mine = place[0], place[1]
    if len(params.shape) == 4:
        params, moments = params.at[0], moments.at[0]
    rows = padded.shape[1] - 2
    band = rows // pieces
    channels = padded.shape[2]
    part = params.shape[1]
    slot = pl.ds(pl.multiple_of(mine * part, part), part)
    kept = slot if final else slice(None)
    for r in range(rows):
        act[r] = padded[0, r + 1]
        cot[r] = padded[1, r + 1, kept, :]
    for image in range(images - 1):
        for s in range(pieces):
            piece = given[image * pieces + s]
            start = (image + 1) * rows + lax.rem(me + s, pieces) * band
            for r in range(band):
                act[start + r] = silu16(piece[0, r])
                cot[start + r] = piece[1, r, kept, :]
    for b in range(3):
        source = cot
        if b != 1:
            source = moved
            for r in range(images * rows):
                moved[r] = lane_shift(cot[r].astype(f32), b - 1).astype(bf16)
        for a in range(3):
            valid = [
                (i * rows + r, i * rows + r + a - 1)
                for i in range(images)
                for r in range(rows)
                if 0 <= r + a - 1 < rows
            ]
            left = jnp.concatenate([source[r] for r, _ in valid], axis=1)
            right = jnp.concatenate([act[r] for _, r in valid], axis=1)
            grad = lax.dot_general(
                left, right, (((1,), (1,)), ((), ())), preferred_element_type=f32
            )
            tap = 3 * a + b
            if final:
                mine_grad = grad
            else:
                total[...] = grad
                mine_grad = total[slot, :]
            step = momentum_decay * moments[tap] + scale * mine_grad
            moments_out[tap] = step
            params_out[tap] = params[tap] - learn_rate * step
            if not final:
                cols = slice(a * channels, (a + 1) * channels)
                step = momentum_decay * speed[b, :, cols].astype(f32) + scale * grad
                speed_out[b, :, cols] = step.astype(bf16)
                fresh = weights[b, :, cols].astype(f32) - (learn_rate * scale) * step
                weights_out[b, :, cols] = fresh.astype(bf16)
                back = slice((2 - a) * channels, (3 - a) * channels)
                flip_out[2 - b, :, back] = fresh.T.astype(bf16)


def assemble(sections, pieces, flipping, place, *refs):
    count = sections * pieces
    given = refs[:count]
    out = refs[count]
    part, channels = given[0].shape[1:]
    me, at = place[0], place[2]
    for d in range(sections):
        for s in range(pieces):
            owner = lax.rem(at + d, sections) * pieces + lax.rem(me + s, pieces)
            slot = pl.ds(pl.multiple_of(owner * part, part), part)
            for a in range(3):
                for b in range(3):
                    out[b, slot, a * channels : (a + 1) * channels] = given[d * pieces + s][3 * a + b]
    if flipping:
        flip = refs[count + 1]
        for a in range(3):
            for b in range(3):
                block = out[b, :, a * channels : (a + 1) * channels].astype(f32)
                flip[2 - b, :, (2 - a) * channels : (3 - a) * channels] = block.T.astype(bf16)


def call(body, outs, inputs, flops, scratch=(), slot=None, aliases=0, read=None):
    size = sum(math.prod(x.shape) * x.dtype.itemsize for x in list(inputs) + list(outs))
    extra, in_out = {}, {}
    out_specs = [VMEM] * len(outs)

    def half(x, which):
        return pl.BlockSpec((1,) + x.shape[1:], lambda i, n=len(x.shape): (which,) + (0,) * (n - 1))

    if slot is not None or read is not None:
        extra["grid"] = (1,)
    if slot is not None:
        out_specs = [half(x, slot) for x in outs]
        in_out = {len(inputs) - aliases + k: k for k in range(aliases)}
    in_specs = [SMEM] + [VMEM] * (len(inputs) - 1 - aliases)
    if read is not None:
        in_specs[-2:] = [half(x, read) for x in inputs[-2:]]
    in_specs += [pl.BlockSpec(memory_space=pl.ANY)] * aliases
    return pl.pallas_call(
        body,
        out_shape=outs,
        in_specs=in_specs,
        out_specs=out_specs,
        scratch_shapes=list(scratch),
        input_output_aliases=in_out,
        compiler_params=pltpu.CompilerParams(vmem_limit_bytes=32 * 1024 * 1024),
        cost_estimate=pl.CostEstimate(flops=flops, bytes_accessed=size, transcendentals=0),
        **extra,
    )(*inputs)


def local(inbox, fresh, params, moments):
    channels, band, width = inbox.shape[3:]
    scale = 1.0 / math.sqrt(9 * channels)
    pieces = lax.axis_size("spatial")
    images = lax.axis_size("dp")
    rows = band * pieces
    ticks = fresh.shape[0] + 1
    sections = lax.axis_size("section")
    top_section = lax.axis_index("section") == sections - 1
    me, at = lax.axis_index("spatial"), lax.axis_index("dp")
    place = jnp.stack([me, at * pieces + me, at]).astype(jnp.int32)
    shape = jax.ShapeDtypeStruct
    message = shape((2, band, channels, width), bf16)
    padded = shape((2, rows + 2, channels, width), bf16)
    block = shape((3, channels, 3 * channels), bf16)
    conv_flops = 2 * 2 * 9 * channels * channels * rows * width

    def rowwise(stack, members):
        return jnp.stack([jnp.swapaxes(stack[m, 0], 0, 1) for m in members])

    def abroad(shard):
        return around(shard, "dp")[1:]

    def spread(parts):
        return [q for p in parts for q in around(p, "spatial")]

    def assembled(parts, flipping):
        body = functools.partial(assemble, images, pieces, flipping)
        return call(body, [block] * (2 if flipping else 1), [place] + parts, channels**3)

    def one(first, second, kernel, flip):
        inputs = [place] + first + second + [kernel, flip]
        scratch = [pltpu.VMEM((rows, channels, width), bf16), pltpu.VMEM((2, rows, channels, width), bf16)]
        return call(
            functools.partial(stage_one, pieces), [padded, padded, message], inputs, conv_flops, scratch
        )

    def two(padded_b, first, second, kernel, flip):
        inputs = [place, padded_b, first, second, kernel, flip]
        return call(stage_two, [message], inputs, conv_flops // pieces)[0]

    def learn(padded_own, others, state, slot=None, pair=(), read=None):
        weights, speed, own_params, own_moments = state
        final = slot is not None
        share = own_params.shape[-2]
        depths = (channels, share, share) if final else (channels,) * 3
        scratch = [pltpu.VMEM((images * rows, depth, width), bf16) for depth in depths]
        inputs = [place, padded_own] + others
        if final:
            outs = [shape((2,) + own_params.shape, f32)] * 2
            inputs += [own_params, own_moments, *pair]
        else:
            inputs += [weights, speed, own_params, own_moments]
            outs = [block] * 3 + [shape(own_params.shape[-3:], f32)] * 2
            scratch += [pltpu.VMEM((channels, channels), f32)]
        body = functools.partial(update, pieces, images, final, scale)
        flops = 2 * 9 * channels * channels * rows * width * images
        return call(body, outs, inputs, flops, scratch, slot, len(pair), read)

    kernel_g = (params[0, 1] * scale).astype(bf16)
    far_g = abroad(kernel_g)
    own_g = around(kernel_g, "spatial")
    kernel_f = (params[0, 0] * scale).astype(bf16)
    far_f = abroad(kernel_f)
    own_f = around(kernel_f, "spatial")
    first = rowwise(inbox[0], (0, 3))
    second = rowwise(inbox[0], (1, 2))
    first, second = lax.optimization_barrier((first, second))
    first_all = around(first, "spatial")
    second_all = around(second, "spatial")
    far_a = abroad(first)
    speeds = moments[0].astype(bf16)
    far_mg = abroad(speeds[1])
    far_mf = abroad(speeds[0])
    own_mg, own_mf = around(speeds[1], "spatial"), around(speeds[0], "spatial")
    far_g = spread(far_g)
    weights_g, flip_g = assembled(own_g + far_g, True)
    far_f = spread(far_f)
    weights_f, flip_f = assembled(own_f + far_f, True)
    params_f = params_g = params[0]
    moments_f = moments_g = moments[0]
    down = [(i, i - 1) for i in range(1, sections)]
    for tick in range(ticks):
        final = tick == ticks - 1
        padded_a, padded_b, middle = one(first_all, second_all, weights_g, flip_g)
        if not final:
            second = lax.ppermute(middle, "section", down)
        far_b = abroad(middle)
        if tick == 1:
            held, _ = lax.optimization_barrier((held, middle))
            weights_f, flip_f, speed_f, params_f, moments_f = learn(
                held, others_f, (weights_f, speed_f, params_f, moments_f), read=0
            )
        last = two(padded_b, first, middle, weights_f, flip_f)
        if not final:
            following = lax.ppermute(last, "section", down)
            given, _ = lax.optimization_barrier((fresh, last))
            later = lax.optimization_barrier(
                (rowwise(given[tick], (0, 3)), rowwise(given[tick], (1, 2)))
            )
        else:
            sent = jnp.stack([last[0], middle[0], middle[1], last[1]])
            outbox = jnp.swapaxes(sent, 1, 2)[None, :, None]
            outbox = with_layout_constraint(outbox, Layout(tuple(range(outbox.ndim))))
            outbox, far_a = lax.optimization_barrier((outbox, far_a))
        others_g = spread(far_a)
        if tick == 0:
            far_mg = spread(far_mg)
            (speed_g,) = assembled(own_mg + far_mg, False)
        state_g = (None, None, params_g, moments_g) if final else (
            weights_g, speed_g, params_g, moments_g
        )
        if final:
            pair = learn(padded_a, others_g, state_g, 1)
        else:
            weights_g, flip_g, speed_g, params_g, moments_g = learn(
                padded_a, others_g, state_g, read=1 if tick == 0 else None
            )
        if not final:
            second = jnp.where(top_section, later[1], second)
            second_all = around(second, "spatial")
        others_f = spread(far_b)
        if not final:
            first = jnp.where(top_section, later[0], following)
            first_all = around(first, "spatial")
            far_a = abroad(first)
        if tick == 0:
            far_mf = spread(far_mf)
            (speed_f,) = assembled(own_mf + far_mf, False)
        if tick == 0:
            held = padded_b
            continue
        if final:
            state_f = (None, None, params_f, moments_f)
            params_out, moments_out = learn(padded_b, others_f, state_f, 0, pair)
        else:
            state_f = (weights_f, speed_f, params_f, moments_f)
            weights_f, flip_f, speed_f, params_f, moments_f = learn(padded_b, others_f, state_f)
    return outbox, params_out[None], moments_out[None]


def solution(mesh):
    placed = (
        P("section", None, "dp", None, "spatial", None),
        P(None, None, "dp", None, "spatial", None),
        P("section", None, None, ("dp", "spatial"), None),
        P("section", None, None, ("dp", "spatial"), None),
    )
    return jax.shard_map(
        local,
        mesh=mesh,
        in_specs=placed,
        out_specs=(
            P("section", None, "dp", None, "spatial", None),
            P("section", None, None, ("dp", "spatial"), None),
            P("section", None, None, ("dp", "spatial"), None),
        ),
        check_vma=False,
    )
```

```python
import functools
import math

import jax
import jax.numpy as jnp
from jax import lax
from jax.experimental import pallas as pl
from jax.experimental.pallas import tpu as pltpu
from jax.experimental.layout import Layout, with_layout_constraint
from jax.sharding import PartitionSpec as P


learn_rate = 0.05
momentum_decay = 0.9

VMEM = pl.BlockSpec(memory_space=pltpu.VMEM)
SMEM = pl.BlockSpec(memory_space=pltpu.SMEM)
f32 = jnp.float32
bf16 = jnp.bfloat16


def ring(axis, shift):
    count = lax.axis_size(axis)
    return [((i + shift) % count, i) for i in range(count)]


def around(shard, axis):
    return [shard] + [
        lax.ppermute(shard, axis, ring(axis, k)) for k in range(1, lax.axis_size(axis))
    ]


def silu_slope(value):
    sigma = jax.nn.sigmoid(value)
    return sigma * (1.0 + value * (1.0 - sigma))


def silu16(value):
    value = value.astype(f32)
    return (value * jax.nn.sigmoid(value)).astype(bf16)


def lane_shift(value, by):
    width = value.shape[-1]
    moved = pltpu.roll(value, by % width, 1)
    lane = lax.broadcasted_iota(jnp.int32, value.shape, 1)
    edge = 0 if by > 0 else width - 1
    return jnp.where(lane == edge, jnp.zeros_like(moved), moved)


def conv_rows(load, count, kernel):
    stacked = jnp.concatenate(
        [jnp.concatenate([load(r + a) for r in range(count)], axis=1) for a in range(3)], axis=0
    )
    depth = kernel.shape[1]
    joined = jnp.dot(
        kernel[...].reshape(3 * depth, kernel.shape[2]), stacked, preferred_element_type=f32
    )
    sums = [joined[b * depth : (b + 1) * depth] for b in range(3)]
    width = stacked.shape[1] // count
    rows = []
    for r in range(count):
        left, middle, right = (s[:, r * width : (r + 1) * width] for s in sums)
        rows.append(middle + lane_shift(left, 1) + lane_shift(right, -1))
    return rows


def stage_one(pieces, images, place, *refs):
    first, second = refs[:pieces], refs[pieces : 2 * pieces]
    kernel, flip, padded_a, padded_b, own = refs[2 * pieces : 2 * pieces + 5]
    packed = refs[2 * pieces + 5 : -2]
    raw, other = refs[-2:]
    band = first[0].shape[1]
    rows = band * pieces
    zero = jnp.zeros(padded_a.shape[2:], bf16)
    for member in range(2):
        for edge in (0, rows + 1):
            padded_a[member, edge] = zero
            padded_b[member, edge] = zero
    me = place[0]
    for s in range(pieces):
        start = lax.rem(me + s, pieces) * band
        for r in range(band):
            half = first[s][0, r]
            raw[start + r] = half
            padded_a[0, start + r + 1] = silu16(half)
            padded_a[1, start + r + 1] = first[s][1, r]
            for member in range(2):
                other[member, start + r] = second[s][member, r]
    moved = conv_rows(lambda i: padded_a[0, i], rows, kernel)
    for r in range(rows):
        prev = (other[0, r].astype(f32) - moved[r]).astype(bf16)
        other[0, r] = prev
        padded_b[0, r + 1] = silu16(prev)
    moved = conv_rows(lambda i: padded_a[1, i], rows, flip)
    for r in range(rows):
        slope = silu_slope(raw[r].astype(f32))
        back = (other[1, r].astype(f32) + slope * moved[r]).astype(bf16)
        other[1, r] = back
        padded_b[1, r + 1] = back
    for member in range(2):
        for r in range(band):
            own[member, r] = other[member, me * band + r]
    channels = own.shape[2]
    chunk = channels // images
    for k, out in enumerate(packed):
        goal = lax.rem(place[2] - (k + 1) + images, images)
        for r in range(band):
            out[r, :channels] = other[0, me * band + r]
            out[r, channels:] = other[1, me * band + r, pl.ds(pl.multiple_of(goal * chunk, chunk), chunk), :]


def stage_two(place, padded, first, second, kernel, flip, out):
    band = first.shape[1]
    base = place[0] * band
    moved = conv_rows(lambda i: padded[0, base + i], band, kernel)
    for r in range(band):
        out[0, r] = (first[0, r].astype(f32) - moved[r]).astype(bf16)
    moved = conv_rows(lambda i: padded[1, base + i], band, flip)
    for r in range(band):
        slope = silu_slope(second[0, r].astype(f32))
        out[1, r] = (first[1, r].astype(f32) + slope * moved[r]).astype(bf16)


def update(pieces, images, final, keep_speed, scale, place, padded, *refs):
    count = pieces * (images - 1)
    given, refs = refs[:count], list(refs[count:])
    act, cot, total = refs[-3:]
    if final:
        params, moments = refs[:2]
        params_out, moments_out = (ref.at[0] for ref in refs[-5:-3])
    else:
        weights, speed, params, moments, weights_out, flip_out = refs[:6]
        speed_out = refs[6] if keep_speed else None
        params_out, moments_out = refs[-5:-3]
    me, mine = place[0], place[1]
    if len(params.shape) == 4:
        params, moments = params.at[0], moments.at[0]
    rows = padded.shape[1] - 2
    band = rows // pieces
    channels = padded.shape[2]
    part = params.shape[1]
    slot = pl.ds(pl.multiple_of(mine * part, part), part)
    kept = slot if final else slice(None)

    def place_row(row, value):
        cot[1, row] = value
        value = value.astype(f32)
        cot[0, row] = lane_shift(value, -1).astype(bf16)
        cot[2, row] = lane_shift(value, 1).astype(bf16)

    for r in range(rows):
        act[r] = padded[0, r + 1]
        place_row(r, padded[1, r + 1, kept, :])
    for image in range(images - 1):
        for s in range(pieces):
            piece = given[image * pieces + s]
            start = (image + 1) * rows + lax.rem(me + s, pieces) * band
            for r in range(band):
                if len(piece.shape) == 3:
                    act[start + r] = silu16(piece[r, :channels])
                    near = pl.ds(pl.multiple_of(channels + me * part, part), part)
                    place_row(start + r, piece[r, near, :])
                else:
                    act[start + r] = silu16(piece[0, r])
                    place_row(start + r, piece[1, r, kept, :])
    depth = cot.shape[2]
    for a in range(3):
        valid = [
            (i * rows + r, i * rows + r + a - 1)
            for i in range(images)
            for r in range(rows)
            if 0 <= r + a - 1 < rows
        ]
        left = jnp.concatenate(
            [jnp.concatenate([cot[b, r] for r, _ in valid], axis=1) for b in range(3)], axis=0
        )
        right = jnp.concatenate([act[r] for _, r in valid], axis=1)
        total[...] = lax.dot_general(
            left, right, (((1,), (1,)), ((), ())), preferred_element_type=f32
        )
        for b in range(3):
            tap = 3 * a + b
            if final:
                mine_grad = total[b * depth : (b + 1) * depth, :]
            else:
                mine_grad = total[pl.ds(pl.multiple_of(b * depth + mine * part, part), part), :]
            step = momentum_decay * moments[tap] + scale * mine_grad
            moments_out[tap] = step
            params_out[tap] = params[tap] - learn_rate * step
            if not final:
                cols = slice(a * channels, (a + 1) * channels)
                grad = total[b * depth : (b + 1) * depth, :]
                step = momentum_decay * speed[b, :, cols].astype(f32) + scale * grad
                if keep_speed:
                    speed_out[b, :, cols] = step.astype(bf16)
                fresh = weights[b, :, cols].astype(f32) - (learn_rate * scale) * step
                fresh = fresh.astype(bf16)
                weights_out[b, :, cols] = fresh
                back = slice((2 - a) * channels, (3 - a) * channels)
                flip_out[2 - b, :, back] = fresh.T


def assemble(sections, pieces, flipping, place, *refs):
    count = sections * pieces
    given = refs[:count]
    out = refs[count]
    part, channels = given[0].shape[1:]
    me, at = place[0], place[2]
    for d in range(sections):
        for s in range(pieces):
            owner = lax.rem(at + d, sections) * pieces + lax.rem(me + s, pieces)
            slot = pl.ds(pl.multiple_of(owner * part, part), part)
            for a in range(3):
                for b in range(3):
                    out[b, slot, a * channels : (a + 1) * channels] = given[d * pieces + s][3 * a + b]
    if flipping:
        flip = refs[count + 1]
        for a in range(3):
            for b in range(3):
                block = out[b, :, a * channels : (a + 1) * channels]
                flip[2 - b, :, (2 - a) * channels : (3 - a) * channels] = block.T


def call(body, outs, inputs, flops, scratch=(), slot=None, aliases=0, read=None):
    size = sum(math.prod(x.shape) * x.dtype.itemsize for x in list(inputs) + list(outs))
    extra, in_out = {}, {}
    out_specs = [VMEM] * len(outs)

    def half(x, which):
        return pl.BlockSpec((1,) + x.shape[1:], lambda i, n=len(x.shape): (which,) + (0,) * (n - 1))

    if slot is not None or read is not None:
        extra["grid"] = (1,)
    if slot is not None:
        out_specs = [half(x, slot) for x in outs]
        in_out = {len(inputs) - aliases + k: k for k in range(aliases)}
    in_specs = [SMEM] + [VMEM] * (len(inputs) - 1 - aliases)
    if read is not None:
        in_specs[-2:] = [half(x, read) for x in inputs[-2:]]
    in_specs += [pl.BlockSpec(memory_space=pl.ANY)] * aliases
    return pl.pallas_call(
        body,
        out_shape=outs,
        in_specs=in_specs,
        out_specs=out_specs,
        scratch_shapes=list(scratch),
        input_output_aliases=in_out,
        compiler_params=pltpu.CompilerParams(vmem_limit_bytes=(8 + 4 * lax.axis_size("dp")) << 20),
        cost_estimate=pl.CostEstimate(flops=flops, bytes_accessed=size, transcendentals=0),
        **extra,
    )(*inputs)


def local(inbox, fresh, params, moments):
    channels, band, width = inbox.shape[3:]
    scale = 1.0 / math.sqrt(9 * channels)
    pieces = lax.axis_size("spatial")
    images = lax.axis_size("dp")
    rows = band * pieces
    ticks = fresh.shape[0] + 1
    sections = lax.axis_size("section")
    top_section = lax.axis_index("section") == sections - 1
    me, at = lax.axis_index("spatial"), lax.axis_index("dp")
    place = jnp.stack([me, at * pieces + me, at]).astype(jnp.int32)
    shape = jax.ShapeDtypeStruct
    message = shape((2, band, channels, width), bf16)
    padded = shape((2, rows + 2, channels, width), bf16)
    block = shape((3, channels, 3 * channels), bf16)
    conv_flops = 2 * 2 * 9 * channels * channels * rows * width

    def rowwise(stack, members):
        return jnp.stack([jnp.swapaxes(stack[m, 0], 0, 1) for m in members])

    def abroad(shard):
        return around(shard, "dp")[1:]

    def spread(parts):
        return [q for p in parts for q in around(p, "spatial")]

    def assembled(parts, flipping):
        body = functools.partial(assemble, images, pieces, flipping)
        return call(body, [block] * (2 if flipping else 1), [place] + parts, channels**3)

    def one(first, second, kernel, flip, final):
        inputs = [place] + first + second + [kernel, flip]
        scratch = [pltpu.VMEM((rows, channels, width), bf16), pltpu.VMEM((2, rows, channels, width), bf16)]
        outs = [padded, padded, message]
        if final:
            outs += [shape((band, channels + channels // images, width), bf16)] * (images - 1)
        body = functools.partial(stage_one, pieces, images)
        return call(body, outs, inputs, conv_flops, scratch)

    def two(padded_b, first, second, kernel, flip):
        inputs = [place, padded_b, first, second, kernel, flip]
        return call(stage_two, [message], inputs, conv_flops // pieces)[0]

    def learn(padded_own, others, state, slot=None, pair=(), read=None, keep_speed=True):
        weights, speed, own_params, own_moments = state
        final = slot is not None
        share = own_params.shape[-2]
        depth = share if final else channels
        count = images * rows
        scratch = [
            pltpu.VMEM((count, channels, width), bf16),
            pltpu.VMEM((3, count, depth, width), bf16),
            pltpu.VMEM((3 * depth, channels), f32),
        ]
        inputs = [place, padded_own] + others
        if final:
            outs = [shape((2,) + own_params.shape, f32)] * 2
            inputs += [own_params, own_moments, *pair]
        else:
            inputs += [weights, speed, own_params, own_moments]
            outs = [block] * (3 if keep_speed else 2) + [shape(own_params.shape[-3:], f32)] * 2
        body = functools.partial(update, pieces, images, final, keep_speed, scale)
        flops = 2 * 9 * channels * channels * rows * width * images
        results = call(body, outs, inputs, flops, scratch, slot, len(pair), read)
        if final or keep_speed:
            return results
        return [*results[:2], None, *results[2:]]

    kernel_g = (params[0, 1] * scale).astype(bf16)
    far_g = abroad(kernel_g)
    own_g = around(kernel_g, "spatial")
    later_params, _ = lax.optimization_barrier((params, kernel_g))
    kernel_f = (later_params[0, 0] * scale).astype(bf16)
    far_f = abroad(kernel_f)
    own_f = around(kernel_f, "spatial")
    first = rowwise(inbox[0], (0, 3))
    second = rowwise(inbox[0], (1, 2))
    first, second = lax.optimization_barrier((first, second))
    first_all = around(first, "spatial")
    second_all = around(second, "spatial")
    far_a = abroad(first)
    speeds = moments[0].astype(bf16)
    far_mg = abroad(speeds[1])
    far_mf = abroad(speeds[0])
    own_mg, own_mf = around(speeds[1], "spatial"), around(speeds[0], "spatial")
    far_g = spread(far_g)
    weights_g, flip_g = assembled(own_g + far_g, True)
    far_f = spread(far_f)
    weights_f, flip_f = assembled(own_f + far_f, True)
    params_f = params_g = params[0]
    moments_f = moments_g = moments[0]
    down = [(i, i - 1) for i in range(1, sections)]
    for tick in range(ticks):
        final = tick == ticks - 1
        padded_a, padded_b, middle, *packed = one(first_all, second_all, weights_g, flip_g, final)
        if not final:
            second = lax.ppermute(middle, "section", down)
        if final:
            far_b = [
                lax.ppermute(p, "dp", ring("dp", k + 1)) for k, p in enumerate(packed)
            ]
        else:
            far_b = abroad(middle)
        if tick == 1:
            held, _ = lax.optimization_barrier((held, middle))
            weights_f, flip_f, speed_f, params_f, moments_f = learn(
                held, others_f, (weights_f, speed_f, params_f, moments_f), read=0
            )
        last = two(padded_b, first, middle, weights_f, flip_f)
        if not final:
            following = lax.ppermute(last, "section", down)
            given, _ = lax.optimization_barrier((fresh, last))
            later = lax.optimization_barrier(
                (rowwise(given[tick], (0, 3)), rowwise(given[tick], (1, 2)))
            )
        else:
            sent = jnp.stack([last[0], middle[0], middle[1], last[1]])
            outbox = jnp.swapaxes(sent, 1, 2)[None, :, None]
            outbox = with_layout_constraint(outbox, Layout(tuple(range(outbox.ndim))))
            outbox, padded_a = lax.optimization_barrier((outbox, padded_a))
        others_g = spread(far_a)
        if tick == 0:
            far_mg = spread(far_mg)
            (speed_g,) = assembled(own_mg + far_mg, False)
        state_g = (None, None, params_g, moments_g) if final else (
            weights_g, speed_g, params_g, moments_g
        )
        if final:
            pair = learn(padded_a, others_g, state_g, 1)
        else:
            weights_g, flip_g, speed_g, params_g, moments_g = learn(
                padded_a, others_g, state_g, read=1 if tick == 0 else None,
                keep_speed=tick < ticks - 2,
            )
        if not final:
            second = jnp.where(top_section, later[1], second)
            second_all = around(second, "spatial")
        others_f = spread(far_b)
        if not final:
            first = jnp.where(top_section, later[0], following)
            first_all = around(first, "spatial")
            far_a = abroad(first)
        if tick == 0:
            far_mf = spread(far_mf)
            (speed_f,) = assembled(own_mf + far_mf, False)
        if tick == 0:
            held = padded_b
            continue
        if final:
            state_f = (None, None, params_f, moments_f)
            params_out, moments_out = learn(padded_b, others_f, state_f, 0, pair)
        else:
            state_f = (weights_f, speed_f, params_f, moments_f)
            weights_f, flip_f, speed_f, params_f, moments_f = learn(
                padded_b, others_f, state_f, keep_speed=tick < ticks - 2
            )
    return outbox, params_out[None], moments_out[None]


def solution(mesh):
    placed = (
        P("section", None, "dp", None, "spatial", None),
        P(None, None, "dp", None, "spatial", None),
        P("section", None, None, ("dp", "spatial"), None),
        P("section", None, None, ("dp", "spatial"), None),
    )
    return jax.shard_map(
        local,
        mesh=mesh,
        in_specs=placed,
        out_specs=(
            P("section", None, "dp", None, "spatial", None),
            P("section", None, None, ("dp", "spatial"), None),
            P("section", None, None, ("dp", "spatial"), None),
        ),
        check_vma=False,
    )
```
